32 devices in a mesh: batch: 2 (over x), w: 4 (over z), h: 4 (over y, core).
Axes of the slice: x: 2, y: 2, z: 4, core: 2. Of those that a mesh axis runs over, the one named last changes fastest.
Arguments:
- images: bfloat16 [32, 1024, 512, 4], P('batch', 'h', 'w'), parts along dimension 0
- down_w1: bfloat16 [3, 3, 4, 64], replicated
- down_b1: float32 [64], replicated
- refine_w1: bfloat16 [3, 3, 64, 64], replicated
- refine_b1: float32 [64], replicated
- down_w2: bfloat16 [3, 3, 64, 128], replicated
- down_b2: float32 [128], replicated
- refine_w2: bfloat16 [3, 3, 128, 128], replicated
- refine_b2: float32 [128], replicated
- down_w3: bfloat16 [3, 3, 128, 256], replicated
- down_b3: float32 [256], replicated
- refine_w3: bfloat16 [3, 3, 256, 256], replicated
- refine_b3: float32 [256], replicated
Outputs:
- output: bfloat16 [32, 128, 64, 256], P('batch', 'h', 'w'), parts along dimension 0
There are 2 independent parts. The reference program is written for one: setup_inputs(seed, part) draws one part's arguments, and reference() takes and returns one part's arrays. A program takes and returns all parts, laid end to end along the dimension named above; an argument that names none is the same for every part.
All inputs are finite; a program needn't handle non-finite values.
Results may differ from the reference program's by a relative error of at most 0.00333018.
Values are sent between devices in bfloat16 or wider.
A program may use at most 1 GiB of HBM per device.

```python
import jax
import jax.numpy as jnp
from jax import lax

BATCH = 16
IMG_H = 1024
IMG_W = 512
CIN = 4
WIDTH = 64

DIM_NUMS = ('NHWC', 'HWIO', 'NHWC')


def conv_weight(rng_key, chan_in, chan_out):
    weight_scale = (2.0 / (9 * chan_in)) ** 0.5
    raw_draw = jax.random.normal(rng_key, (3, 3, chan_in, chan_out), jnp.float32)
    return (raw_draw * weight_scale).astype(jnp.bfloat16)


def setup_inputs(seed: int = 0, part: int = 0) -> dict:
    image_key = jax.random.fold_in(jax.random.key(seed), part)
    key_list = jax.random.split(jax.random.key(seed + 1), 12)
    widths = [CIN, WIDTH, 2 * WIDTH, 4 * WIDTH]
    images = jax.random.normal(image_key, (BATCH, IMG_H, IMG_W, CIN), jnp.float32)
    arrays = {'images': images.astype(jnp.bfloat16)}
    for stage_num in range(3):
        chan_in = widths[stage_num]
        chan_out = widths[stage_num + 1]
        suffix = str(stage_num + 1)
        arrays['down_w' + suffix] = conv_weight(key_list[4 * stage_num], chan_in, chan_out)
        arrays['down_b' + suffix] = 0.3 * jax.random.normal(key_list[4 * stage_num + 1], (chan_out,), jnp.float32)
        arrays['refine_w' + suffix] = conv_weight(key_list[4 * stage_num + 2], chan_out, chan_out)
        arrays['refine_b' + suffix] = 0.3 * jax.random.normal(key_list[4 * stage_num + 3], (chan_out,), jnp.float32)
    return arrays


def periodic_conv(current, weight, bias_vec, stride):
    padded = jnp.pad(current, ((1, 1), (1, 1), (0, 0)), mode='wrap')
    conv_out = lax.conv_general_dilated(padded[None].astype(jnp.float32), weight.astype(jnp.float32), (stride, stride), 'VALID', dimension_numbers=DIM_NUMS)
    return jnp.maximum(conv_out[0] + bias_vec, 0.0).astype(jnp.bfloat16)


def reference(images, down_w1, down_b1, refine_w1, refine_b1, down_w2, down_b2, refine_w2, refine_b2, down_w3, down_b3, refine_w3, refine_b3):
    stages = [(down_w1, down_b1, refine_w1, refine_b1), (down_w2, down_b2, refine_w2, refine_b2), (down_w3, down_b3, refine_w3, refine_b3)]

    def encode_image(one_image):
        current = one_image
        for down_w, down_b, refine_w, refine_b in stages:
            current = periodic_conv(current, down_w, down_b, 2)
            current = periodic_conv(current, refine_w, refine_b, 1)
        return current

    return lax.map(encode_image, images)
```

```python
import functools

import jax
import jax.numpy as jnp
from jax import lax
from jax.experimental import pallas as pl
from jax.experimental.pallas import tpu as pltpu
from jax.sharding import PartitionSpec as P

DIM_NUMS = ('HWNC', 'HWIO', 'HWNC')

TOP, BOT = 16, 8
WINDOWS = 6
STEP = 28
FIRST = -13
OUT_COLS = 14


def next_perm(axis_size):
    return [(src_dev, (src_dev + 1) % axis_size) for src_dev in range(axis_size)]


def prev_perm(axis_size):
    return [(src_dev, (src_dev - 1) % axis_size) for src_dev in range(axis_size)]


def lane_window(pieces, start, width, offset):
    lane = lax.broadcasted_iota(jnp.int32, pieces[0].shape, 1)
    total = None
    for chan, piece in enumerate(pieces):
        shift = (32 * chan + offset - start) % 128
        moved = pltpu.roll(piece, shift, 1) if shift else piece
        if total is None:
            total = moved
        else:
            total = jnp.where(lane >= 32 * chan, moved, total)
    return total


def slab_kernel(top_ref, mid_ref, bot_ref, main_ref, own0_ref, own5_ref, to_next_ref, to_prev_ref, rows_ref):
    step = pl.program_id(0)

    @pl.when(step < TOP // 8)
    def _():
        rows_ref[...] = top_ref[...].astype(jnp.float32)

    @pl.when((step >= TOP // 8) & (step < 34))
    def _():
        rows_ref[...] = mid_ref[...].astype(jnp.float32)

    @pl.when(step == 34)
    def _():
        rows_ref[...] = bot_ref[...].astype(jnp.float32)

    lane = lax.broadcasted_iota(jnp.int32, (16, 128), 1) % 32
    next_rows, prev_rows = [], []
    for row in range(8):
        pieces = [rows_ref[row, chan] for chan in range(4)]
        for win in range(1, 5):
            main_ref[row, win - 1] = lane_window(pieces, FIRST + STEP * win, 32, 0).astype(jnp.bfloat16)
        own0_ref[row] = lane_window(pieces, 0, 16, 13).astype(jnp.bfloat16)
        own5_ref[row] = lane_window(pieces, 127, 1, 0).astype(jnp.bfloat16)
        next_rows.append(lane_window(pieces, 115, 13, 16 * (row % 2)))
        prev_rows.append(lane_window(pieces, 0, 8, 8 * (row % 4)))
    for pair in range(4):
        packed = jnp.where(lane < 16, next_rows[2 * pair], next_rows[2 * pair + 1])
        to_next_ref[pair] = packed.astype(jnp.bfloat16)
    for quad in range(2):
        packed = prev_rows[4 * quad]
        for part in range(1, 4):
            packed = jnp.where(lane >= 8 * part, prev_rows[4 * quad + part], packed)
        to_prev_ref[quad] = packed.astype(jnp.bfloat16)


def make_slabs(top, mid, bot):
    block = (8, 4, 16, 128)
    bf16 = jnp.bfloat16
    return pl.pallas_call(
        slab_kernel,
        grid=(35,),
        in_specs=[
            pl.BlockSpec(block, lambda s: (jnp.minimum(s, 1), 0, 0, 0)),
            pl.BlockSpec(block, lambda s: (jnp.clip(s - 2, 0, 31), 0, 0, 0)),
            pl.BlockSpec(block, lambda s: (0, 0, 0, 0)),
        ],
        out_specs=[
            pl.BlockSpec((8, 4, 16, 128), lambda s: (s, 0, 0, 0)),
            pl.BlockSpec((8, 16, 128), lambda s: (s, 0, 0)),
            pl.BlockSpec((8, 16, 128), lambda s: (s, 0, 0)),
            pl.BlockSpec((4, 16, 128), lambda s: (s, 0, 0)),
            pl.BlockSpec((2, 16, 128), lambda s: (s, 0, 0)),
        ],
        out_shape=[
            jax.ShapeDtypeStruct((280, 4, 16, 128), bf16),
            jax.ShapeDtypeStruct((280, 16, 128), bf16),
            jax.ShapeDtypeStruct((280, 16, 128), bf16),
            jax.ShapeDtypeStruct((140, 16, 128), bf16),
            jax.ShapeDtypeStruct((70, 16, 128), bf16),
        ],
        scratch_shapes=[pltpu.VMEM(block, jnp.float32)],
        cost_estimate=pl.CostEstimate(flops=16_000_000, bytes_accessed=14_000_000, transcendentals=0),
        name='slabs',
    )(top, mid, bot)


def edge_kernel(own0_ref, own5_ref, from_prev_ref, from_next_ref, out_ref):
    lane = lax.broadcasted_iota(jnp.int32, (16, 128), 1) % 32
    for row in range(8):
        left = from_prev_ref[row // 2].astype(jnp.float32)
        if row % 2:
            left = pltpu.roll(left, 128 - 16, 1)
        own0 = own0_ref[row].astype(jnp.float32)
        out_ref[row, 0] = jnp.where(lane < 13, left, own0).astype(jnp.bfloat16)
        right = from_next_ref[row // 4].astype(jnp.float32)
        right = pltpu.roll(right, (1 - 8 * (row % 4)) % 128, 1)
        own5 = own5_ref[row].astype(jnp.float32)
        out_ref[row, 1] = jnp.where(lane < 1, own5, right).astype(jnp.bfloat16)


def make_edges(own0, own5, from_prev, from_next):
    return pl.pallas_call(
        edge_kernel,
        grid=(35,),
        in_specs=[
            pl.BlockSpec((8, 16, 128), lambda s: (s, 0, 0)),
            pl.BlockSpec((8, 16, 128), lambda s: (s, 0, 0)),
            pl.BlockSpec((4, 16, 128), lambda s: (s, 0, 0)),
            pl.BlockSpec((2, 16, 128), lambda s: (s, 0, 0)),
        ],
        out_specs=pl.BlockSpec((8, 2, 16, 128), lambda s: (s, 0, 0, 0)),
        out_shape=jax.ShapeDtypeStruct((280, 2, 16, 128), jnp.bfloat16),
        cost_estimate=pl.CostEstimate(flops=4_000_000, bytes_accessed=8_000_000, transcendentals=0),
        name='edges',
    )(own0, own5, from_prev, from_next)


def first_kernel(counts, slab_ref, toep_ref, bias_ref, out_ref):
    base = 12 * pl.program_id(0) + 3
    wins = len(counts)
    lhs = []
    for row in range(6):
        for win in range(wins):
            taps = [slab_ref[base + 2 * row + tap, win] for tap in range(3)]
            lhs.append(jnp.concatenate(taps, axis=-1))
    lhs = jnp.concatenate(lhs, axis=0)
    bias = bias_ref[...]
    for chunk in range(4):
        width = 256 if chunk < 3 else 128
        acc = jnp.dot(lhs, toep_ref[:, 256 * chunk:256 * chunk + width], preferred_element_type=jnp.float32)
        acc = jnp.maximum(acc + bias[:, :width], 0.0).astype(jnp.bfloat16)
        acc = acc.reshape(6, wins, 16, width)
        offset = 0
        for win in range(wins):
            for half in range(width // 128):
                pair = 2 * chunk + half
                if pair < counts[win]:
                    for row in range(6):
                        out_ref[row // 2, offset + pair, :, 128 * (row % 2):128 * (row % 2) + 128] = acc[row, win, :, 128 * half:128 * half + 128]
            offset += counts[win]


def first_conv(slabs, toep, bias, counts):
    cols = sum(counts)
    return pl.pallas_call(
        functools.partial(first_kernel, counts),
        grid=(23,),
        in_specs=[
            pl.BlockSpec(slabs.shape, lambda s: (0, 0, 0, 0), pipeline_mode=pl.Buffered(1)),
            pl.BlockSpec((384, 896), lambda s: (0, 0), pipeline_mode=pl.Buffered(1)),
            pl.BlockSpec((1, 256), lambda s: (0, 0)),
        ],
        out_specs=pl.BlockSpec((3, cols, 16, 256), lambda s: (s, 0, 0, 0)),
        out_shape=jax.ShapeDtypeStruct((69, cols, 16, 256), jnp.bfloat16),
        cost_estimate=pl.CostEstimate(flops=2 * 2208 * len(counts) * 512 * 1024, bytes_accessed=20_000_000, transcendentals=0),
        name='first',
    )(slabs, toep, bias)


def pack_first(weight):
    cols = []
    for out_col in range(OUT_COLS):
        cols.append(jnp.pad(weight, ((0, 0), (2 * out_col, 29 - 2 * out_col), (0, 0), (0, 0))))
    stacked = jnp.concatenate(cols, axis=-1)
    return stacked.transpose(0, 2, 1, 3).reshape(384, 64 * OUT_COLS)


def pack_refine1(weight):
    wide = jnp.pad(weight, ((1, 1), (1, 1), (0, 0), (0, 0)))
    pieces = [wide[1 - r:5 - r, 1 - c:5 - c] for r in range(2) for c in range(2)]
    joined = jnp.concatenate(pieces, axis=-1)
    return joined.reshape(2, 2, 2, 2, 64, 256).transpose(0, 2, 1, 3, 4, 5).reshape(2, 2, 256, 256)


def pack_down2(weight):
    wide = jnp.pad(weight, ((0, 1), (2, 3), (0, 0), (0, 0)))
    joined = jnp.concatenate([wide[:, 2:8], wide[:, 0:6]], axis=-1)
    return joined.reshape(2, 2, 3, 2, 64, 256).transpose(0, 2, 1, 3, 4, 5).reshape(2, 3, 256, 256)


def pack_refine2(weight):
    wide = jnp.pad(weight, ((0, 0), (1, 1), (0, 0), (0, 0)))
    joined = jnp.concatenate([wide[:, 1:5], wide[:, 0:4]], axis=-1)
    return joined.reshape(3, 2, 256, 256)


def pack_down3(weight):
    return jnp.pad(weight, ((0, 0), (1, 0), (0, 0), (0, 0))).reshape(3, 2, 256, 256)


def conv(x, weight, bias, strides=(1, 1), pad_left=0):
    out = lax.conv_general_dilated(x, weight, strides, ((0, 0), (pad_left, 0)), dimension_numbers=DIM_NUMS, preferred_element_type=jnp.float32)
    return lax.optimization_barrier(jnp.maximum(out + bias, 0.0).astype(jnp.bfloat16))


def solution(mesh):
    h_count = mesh.shape['h']
    w_count = mesh.shape['w']
    tile_spec = P('batch', 'h', 'w', None)

    def per_device(images, dw1, db1, rw1, rb1, dw2, db2, rw2, rb2, dw3, db3, rw3, rb3):
        native = images.transpose(0, 1, 3, 2)
        top = lax.ppermute(native[:, -TOP:], 'h', next_perm(h_count))
        bot = lax.ppermute(native[:, :BOT], 'h', prev_perm(h_count))
        mid = native.transpose(1, 2, 0, 3)
        main, own0, own5, to_next, to_prev = make_slabs(top.transpose(1, 2, 0, 3), mid, bot.transpose(1, 2, 0, 3))
        from_prev = lax.ppermute(to_next, 'w', next_perm(w_count))
        from_next = lax.ppermute(to_prev, 'w', prev_perm(w_count))
        toep = pack_first(dw1)
        bias1 = jnp.tile(db1, 4).reshape(1, 256)
        y1_main = first_conv(main, toep, bias1, (7, 7, 7, 7))
        edges = make_edges(own0, own5, from_prev, from_next)
        y1_edge = first_conv(edges, toep, bias1, (7, 2))
        y1 = jnp.concatenate([y1_edge[:, :7], y1_main, y1_edge[:, 7:]], axis=1)
        z1 = conv(y1, pack_refine1(rw1), jnp.tile(rb1, 4))
        y2 = conv(z1, pack_down2(dw2), jnp.tile(db2, 2), (1, 2), 1)
        z2 = conv(y2, pack_refine2(rw2), jnp.tile(rb2, 2))
        y3 = conv(z2, pack_down3(dw3), db3, (2, 1))
        top_row = lax.ppermute(y3[-1:], 'h', next_perm(h_count))
        bottom_row = lax.ppermute(y3[:1], 'h', prev_perm(h_count))
        tall = jnp.concatenate([top_row, y3, bottom_row], axis=0)
        left_col = lax.ppermute(tall[:, -1:], 'w', next_perm(w_count))
        right_col = lax.ppermute(tall[:, :1], 'w', prev_perm(w_count))
        full = jnp.concatenate([left_col, tall, right_col], axis=1)
        z3 = conv(full, rw3, rb3)
        return z3.transpose(2, 0, 1, 3)

    in_specs = (tile_spec,) + (P(),) * 12
    return jax.shard_map(per_device, mesh=mesh, in_specs=in_specs, out_specs=tile_spec, check_vma=False)
```

```python
import jax
import jax.numpy as jnp
from jax import lax
from jax.experimental.layout import Layout, with_layout_constraint
from jax.experimental import pallas as pl
from jax.experimental.pallas import tpu as pltpu
from jax.sharding import PartitionSpec as P


DIM_NUMS = ('HWNC', 'HWIO', 'HWNC')

TOP, MID, BOT = 24, 256, 16
ROWS = TOP + MID + BOT
PAIRS = 75
STEPS = 3
STEP = 28
FIRST = -13
OUT_COLS = 14


def next_perm(axis_size):
    return [(src_dev, (src_dev + 1) % axis_size) for src_dev in range(axis_size)]


def prev_perm(axis_size):
    return [(src_dev, (src_dev - 1) % axis_size) for src_dev in range(axis_size)]


def lane_window(pieces, start, offset):
    lane = lax.broadcasted_iota(jnp.int32, pieces[0].shape, 1)
    total = None
    for chan, piece in enumerate(pieces):
        shift = (32 * chan + offset - start) % 128
        moved = pltpu.roll(piece, shift, 1) if shift else piece
        total = moved if total is None else jnp.where(lane >= 32 * chan, moved, total)
    return total


def for_quads(sources, body):
    first = 0
    for source in sources:
        quads = source.shape[0] // 4

        @pl.loop(0, quads)
        def _(quad, source=source, first=first):
            rows = [[source[4 * quad + row, chan] for chan in range(4)] for row in range(4)]
            body(first + quad, rows)

        first += quads


def pack_kernel(top_ref, mid_ref, bot_ref, to_next_ref, to_prev_ref):
    lane = lax.broadcasted_iota(jnp.int32, (16, 128), 1) % 32

    def body(quad, rows):
        last = [lane_window(rows[row], 115, 16 * (row % 2)) for row in range(4)]
        to_next_ref[2 * quad] = jnp.where(lane < 16, last[0], last[1])
        to_next_ref[2 * quad + 1] = jnp.where(lane < 16, last[2], last[3])
        packed = lane_window(rows[0], 0, 0)
        for row in range(1, 4):
            packed = jnp.where(lane >= 8 * row, lane_window(rows[row], 0, 8 * row), packed)
        to_prev_ref[quad] = packed

    for_quads((top_ref, mid_ref, bot_ref), body)


def pack_halo(top, mid, bot):
    return pl.pallas_call(
        pack_kernel,
        out_shape=[
            jax.ShapeDtypeStruct((ROWS // 2, 16, 128), jnp.bfloat16),
            jax.ShapeDtypeStruct((ROWS // 4, 16, 128), jnp.bfloat16),
        ],
        cost_estimate=pl.CostEstimate(flops=8_000_000, bytes_accessed=6_000_000, transcendentals=0),
        name='pack',
    )(top, mid, bot)


def product(slab_ref, base, rows, windows, toep_ref, bias, store):
    lhs = []
    for row in range(rows):
        for win, _ in windows:
            taps = [slab_ref[base + 2 * row + tap, win] for tap in range(3)]
            lhs.append(jnp.concatenate(taps, axis=-1))
    lhs = jnp.concatenate(lhs, axis=0)
    most = max(count for _, count in windows)
    for chunk in range((most + 1) // 2):
        width = min(256, 128 * (most - 2 * chunk))
        acc = jnp.dot(lhs, toep_ref[:, 256 * chunk:256 * chunk + width], preferred_element_type=jnp.float32)
        acc = jnp.maximum(acc + bias[:, :width], 0.0).astype(jnp.bfloat16)
        acc = acc.reshape(rows, len(windows), 16, width)
        for index, (win, count) in enumerate(windows):
            for half in range(width // 128):
                pair = 2 * chunk + half
                if pair < count:
                    for row in range(rows):
                        store(row, win, pair, acc[row, index, :, 128 * half:128 * half + 128])


def main_kernel(top_ref, mid_ref, bot_ref, toep_ref, bias_ref, out_ref, own0_ref, own5_ref, slab_ref):
    step = pl.program_id(0)

    @pl.when(step == 0)
    def _():
        def body(quad, rows):
            for row in range(4):
                index = 4 * quad + row
                for win in range(4):
                    slab_ref[index, win] = lane_window(rows[row], FIRST + STEP * (win + 1), 0)
                own0_ref[index] = lane_window(rows[row], 0, 13)
                own5_ref[index] = lane_window(rows[row], 127, 0)

        for_quads((top_ref, mid_ref, bot_ref), body)
        slab_ref[ROWS:ROWS + 8] = jnp.zeros((8, 4, 16, 128), jnp.bfloat16)

    bias = bias_ref[...]
    group = 5

    @pl.loop(0, PAIRS // STEPS // group)
    def _(part):
        first = group * part

        def store(row, win, pair, value):
            out_ref[first + row // 2, 7 * win + pair, :, 128 * (row % 2):128 * (row % 2) + 128] = value

        base = 4 * (PAIRS // STEPS * step + first) + 3
        product(slab_ref, base, 2 * group, [(win, 7) for win in range(4)], toep_ref, bias, store)


def whole(shape):
    return pl.BlockSpec(shape, lambda s: (0,) * len(shape), pipeline_mode=pl.Buffered(1))


def main_first(top, mid, bot, toep, bias):
    bf16 = jnp.bfloat16
    return pl.pallas_call(
        main_kernel,
        grid=(STEPS,),
        in_specs=[whole(x.shape) for x in (top, mid, bot, toep, bias)],
        out_specs=[
            pl.BlockSpec((PAIRS // STEPS, 28, 16, 256), lambda s: (s, 0, 0, 0)),
            whole((ROWS, 16, 128)),
            whole((ROWS, 16, 128)),
        ],
        out_shape=[
            jax.ShapeDtypeStruct((73, 28, 16, 256), bf16),
            jax.ShapeDtypeStruct((ROWS, 16, 128), bf16),
            jax.ShapeDtypeStruct((ROWS, 16, 128), bf16),
        ],
        scratch_shapes=[pltpu.VMEM((ROWS + 8, 4, 16, 128), bf16)],
        cost_estimate=pl.CostEstimate(flops=2 * 2400 * 4 * 512 * 1024, bytes_accessed=24_000_000, transcendentals=0),
        name='main_first',
    )(top, mid, bot, toep, bias)


def edge_kernel(own0_ref, own5_ref, from_prev_ref, from_next_ref, toep_ref, bias_ref, left_ref, right_ref, slab_ref):
    step = pl.program_id(0)

    @pl.when(step == 0)
    def _():
        lane = lax.broadcasted_iota(jnp.int32, (16, 128), 1) % 32

        @pl.loop(0, ROWS // 4)
        def _(quad):
            for row in range(4):
                index = 4 * quad + row
                left = from_prev_ref[2 * quad + row // 2]
                if row % 2:
                    left = pltpu.roll(left, 128 - 16, 1)
                slab_ref[index, 0] = jnp.where(lane < 13, left, own0_ref[index])
                right = pltpu.roll(from_next_ref[quad], (1 - 8 * row) % 128, 1)
                slab_ref[index, 1] = jnp.where(lane < 1, own5_ref[index], right)

        slab_ref[ROWS:ROWS + 8] = jnp.zeros((8, 2, 16, 128), jnp.bfloat16)

    bias = bias_ref[...]
    base = 4 * (PAIRS // STEPS) * step + 3

    def store(row, win, pair, value):
        ref = right_ref if win else left_ref
        ref[row // 2, pair, :, 128 * (row % 2):128 * (row % 2) + 128] = value

    for window in ((0, 7), (1, 2)):
        product(slab_ref, base, 2 * (PAIRS // STEPS), [window], toep_ref, bias, store)


def edge_first(own0, own5, from_prev, from_next, toep, bias):
    bf16 = jnp.bfloat16
    args = (own0, own5, from_prev, from_next, toep, bias)
    return pl.pallas_call(
        edge_kernel,
        grid=(STEPS,),
        in_specs=[whole(x.shape) for x in args],
        out_specs=[
            pl.BlockSpec((PAIRS // STEPS, 7, 16, 256), lambda s: (s, 0, 0, 0)),
            pl.BlockSpec((PAIRS // STEPS, 2, 16, 256), lambda s: (s, 0, 0, 0)),
        ],
        out_shape=[
            jax.ShapeDtypeStruct((73, 7, 16, 256), bf16),
            jax.ShapeDtypeStruct((73, 2, 16, 256), bf16),
        ],
        scratch_shapes=[pltpu.VMEM((ROWS + 8, 2, 16, 128), bf16)],
        cost_estimate=pl.CostEstimate(flops=2 * 2400 * 512 * 1152, bytes_accessed=12_000_000, transcendentals=0),
        name='edge_first',
    )(*args)


def pack_first(weight):
    cols = []
    for out_col in range(OUT_COLS):
        cols.append(jnp.pad(weight, ((0, 0), (2 * out_col, 29 - 2 * out_col), (0, 0), (0, 0))))
    stacked = jnp.concatenate(cols, axis=-1)
    return stacked.transpose(0, 2, 1, 3).reshape(384, 64 * OUT_COLS)


def pack_refine1(weight):
    wide = jnp.pad(weight, ((1, 1), (1, 1), (0, 0), (0, 0)))
    pieces = [wide[1 - r:5 - r, 1 - c:5 - c] for r in range(2) for c in range(2)]
    joined = jnp.concatenate(pieces, axis=-1)
    return joined.reshape(2, 2, 2, 2, 64, 256).transpose(0, 2, 1, 3, 4, 5).reshape(2, 2, 256, 256)


def pack_down2(weight):
    wide = jnp.pad(weight, ((0, 1), (2, 3), (0, 0), (0, 0)))
    joined = jnp.concatenate([wide[:, 2:8], wide[:, 0:6]], axis=-1)
    return joined.reshape(2, 2, 3, 2, 64, 256).transpose(0, 2, 1, 3, 4, 5).reshape(2, 3, 256, 256)


def pack_refine2(weight):
    wide = jnp.pad(weight, ((0, 0), (1, 1), (0, 0), (0, 0)))
    joined = jnp.concatenate([wide[:, 1:5], wide[:, 0:4]], axis=-1)
    return joined.reshape(3, 2, 256, 256)


def pack_down3(weight):
    return jnp.pad(weight, ((0, 0), (1, 0), (0, 0), (0, 0))).reshape(3, 2, 256, 256)


def conv(x, weight, bias, strides=(1, 1), pads=((0, 0), (0, 0))):
    out = lax.conv_general_dilated(x, weight, strides, pads, dimension_numbers=DIM_NUMS, preferred_element_type=jnp.float32)
    return lax.optimization_barrier(jnp.maximum(out + bias, 0.0).astype(jnp.bfloat16))


def solution(mesh):
    h_count = mesh.shape['h']
    w_count = mesh.shape['w']
    tile_spec = P('batch', 'h', 'w', None)

    def keep(x):
        return with_layout_constraint(x, Layout(major_to_minor=(0, 1, 2, 3)))

    def per_device(images, dw1, db1, rw1, rb1, dw2, db2, rw2, rb2, dw3, db3, rw3, rb3):
        native = images.transpose(0, 1, 3, 2)
        top = keep(lax.ppermute(keep(native[:, -TOP:]), 'h', next_perm(h_count)))
        bot = keep(lax.ppermute(keep(native[:, :BOT]), 'h', prev_perm(h_count)))
        top, mid, bot = (x.transpose(1, 2, 0, 3) for x in (top, native, bot))
        toep = pack_first(dw1)
        bias1 = jnp.tile(db1, 4).reshape(1, 256)
        to_next, to_prev = pack_halo(top, mid, bot)
        to_next, rw1, rb1, dw2, db2, rw2, rb2, dw3 = lax.optimization_barrier((to_next, rw1, rb1, dw2, db2, rw2, rb2, dw3))
        from_prev = lax.ppermute(to_next, 'w', next_perm(w_count))
        from_next = lax.ppermute(to_prev, 'w', prev_perm(w_count))
        y1_main, own0, own5 = main_first(top, mid, bot, toep, bias1)
        y1_left, y1_right = edge_first(own0, own5, from_prev, from_next, toep, bias1)
        y1 = jnp.concatenate([y1_left, y1_main, y1_right], axis=1)
        z1 = conv(y1, pack_refine1(rw1), jnp.tile(rb1, 4))
        y2 = conv(z1, pack_down2(dw2), jnp.tile(db2, 2), (1, 2), ((0, 0), (1, 0)))
        rw2, rb2, dw3 = pack_refine2(rw2), jnp.tile(rb2, 2), pack_down3(dw3)
        y2_edge = jnp.concatenate([y2[:, :3], y2[:, 15:18]], axis=2)
        z2_edge = conv(y2_edge, rw2, rb2)
        y3_edge = conv(z2_edge, dw3, db3, (2, 1))
        y3_left, y3_right = y3_edge[:, :, :16], y3_edge[:, :, 16:]
        from_left = lax.ppermute(y3_right, 'w', next_perm(w_count))
        from_right = lax.ppermute(y3_left, 'w', prev_perm(w_count))
        y2, y3_edge = lax.optimization_barrier((y2, y3_edge))
        z2_mid = conv(y2[:, 2:16], rw2, rb2)
        z2 = jnp.concatenate([z2_edge[:, 1:2, :16], z2_mid, z2_edge[:, 0:1, 16:]], axis=1)
        y3_mid = conv(z2, dw3, db3, (2, 1))
        y3_left, y3_right = y3_edge[:, :, :16], y3_edge[:, :, 16:]
        y3_left = jnp.concatenate([from_left, y3_left], axis=1)
        y3_right = jnp.concatenate([y3_right, from_right], axis=1)
        y3_left, y3_right = lax.optimization_barrier((y3_left, y3_right))
        y3 = jnp.concatenate([y3_left, y3_mid, y3_right], axis=1)
        z3 = conv(y3, rw3, rb3)
        return z3.transpose(2, 0, 1, 3)

    in_specs = (tile_spec,) + (P(),) * 12
    return jax.shard_map(per_device, mesh=mesh, in_specs=in_specs, out_specs=tile_spec, check_vma=False)
```

```python
import functools

import jax
import jax.numpy as jnp
from jax import lax
from jax.experimental import pallas as pl
from jax.experimental.pallas import tpu as pltpu
from jax.sharding import PartitionSpec as P


DIM_NUMS = ('HWNC', 'HWIO', 'HWNC')

TOP, MID, BOT = 24, 256, 16
ROWS = TOP + MID + BOT
PAIRS = 75
STEPS = 3
STEP = 28
FIRST = -13
OUT_COLS = 14


def next_perm(axis_size):
    return [(src_dev, (src_dev + 1) % axis_size) for src_dev in range(axis_size)]


def prev_perm(axis_size):
    return [(src_dev, (src_dev - 1) % axis_size) for src_dev in range(axis_size)]


def lane_window(pieces, start, offset):
    lane = lax.broadcasted_iota(jnp.int32, pieces[0].shape, 1)
    total = None
    for chan, piece in enumerate(pieces):
        shift = (32 * chan + offset - start) % 128
        moved = pltpu.roll(piece, shift, 1) if shift else piece
        total = moved if total is None else jnp.where(lane >= 32 * chan, moved, total)
    return total


def blocked_loop(count, unroll, body):
    @pl.loop(0, count // unroll)
    def _(block):
        for part in range(unroll):
            body(unroll * block + part)

    for index in range(count - count % unroll, count):
        body(index)


def for_quads(sources, unroll, body):
    first = 0
    for source in sources:
        def one(quad, source=source, first=first):
            rows = [[source[4 * quad + row, chan] for chan in range(4)] for row in range(4)]
            body(first + quad, rows)

        blocked_loop(source.shape[0] // 4, unroll, one)
        first += source.shape[0] // 4


def pack_kernel(top_ref, mid_ref, bot_ref, to_next_ref, to_prev_ref):
    lane = lax.broadcasted_iota(jnp.int32, (16, 128), 1) % 32

    def body(quad, rows):
        last = [lane_window(rows[row], 115, 16 * (row % 2)) for row in range(4)]
        to_next_ref[2 * quad] = jnp.where(lane < 16, last[0], last[1])
        to_next_ref[2 * quad + 1] = jnp.where(lane < 16, last[2], last[3])
        packed = lane_window(rows[0], 0, 0)
        for row in range(1, 4):
            packed = jnp.where(lane >= 8 * row, lane_window(rows[row], 0, 8 * row), packed)
        to_prev_ref[quad] = packed

    for_quads((top_ref, mid_ref, bot_ref), 8, body)


def pack_halo(top, mid, bot):
    return pl.pallas_call(
        pack_kernel,
        out_shape=[
            jax.ShapeDtypeStruct((ROWS // 2, 16, 128), jnp.bfloat16),
            jax.ShapeDtypeStruct((ROWS // 4, 16, 128), jnp.bfloat16),
        ],
        cost_estimate=pl.CostEstimate(flops=8_000_000, bytes_accessed=6_000_000, transcendentals=0),
        name='pack',
    )(top, mid, bot)


def product(slab_ref, base, rows, windows, toep_ref, bias, store):
    lhs = []
    for row in range(rows):
        for win, _ in windows:
            taps = [slab_ref[base + 2 * row + tap, win] for tap in range(3)]
            lhs.append(jnp.concatenate(taps, axis=-1))
    lhs = jnp.concatenate(lhs, axis=0)
    most = max(count for _, count in windows)
    for chunk in range((most + 1) // 2):
        width = min(256, 128 * (most - 2 * chunk))
        acc = jnp.dot(lhs, toep_ref[:, 256 * chunk:256 * chunk + width], preferred_element_type=jnp.float32)
        acc = jnp.maximum(acc + bias[:, :width], 0.0).astype(jnp.bfloat16)
        acc = acc.reshape(rows, len(windows), 16, width)
        for index, (win, count) in enumerate(windows):
            for half in range(width // 128):
                pair = 2 * chunk + half
                if pair < count:
                    for row in range(rows):
                        store(row, win, pair, acc[row, index, :, 128 * half:128 * half + 128])


def main_kernel(top_ref, mid_ref, bot_ref, toep_ref, bias_ref, out_ref, own0_ref, own5_ref, slab_ref):
    step = pl.program_id(0)

    @pl.when(step == 0)
    def _():
        def body(quad, rows):
            for row in range(4):
                index = 4 * quad + row
                for win in range(4):
                    slab_ref[index, win] = lane_window(rows[row], FIRST + STEP * (win + 1), 0)
                own0_ref[index] = lane_window(rows[row], 0, 13)
                own5_ref[index] = lane_window(rows[row], 127, 0)

        for_quads((top_ref, mid_ref, bot_ref), 4, body)
        slab_ref[ROWS:ROWS + 8] = jnp.zeros((8, 4, 16, 128), jnp.bfloat16)

    bias = bias_ref[...]
    group = 5

    @pl.loop(0, PAIRS // STEPS // group)
    def _(part):
        first = group * part

        def store(row, win, pair, value):
            out_ref[first + row // 2, 7 * win + pair, :, 128 * (row % 2):128 * (row % 2) + 128] = value

        base = 4 * (PAIRS // STEPS * step + first) + 3
        product(slab_ref, base, 2 * group, [(win, 7) for win in range(4)], toep_ref, bias, store)


def whole(shape):
    return pl.BlockSpec(shape, lambda s: (0,) * len(shape), pipeline_mode=pl.Buffered(1))


def main_first(top, mid, bot, toep, bias):
    bf16 = jnp.bfloat16
    return pl.pallas_call(
        main_kernel,
        grid=(STEPS,),
        in_specs=[whole(x.shape) for x in (top, mid, bot, toep, bias)],
        out_specs=[
            pl.BlockSpec((PAIRS // STEPS, 28, 16, 256), lambda s: (s, 0, 0, 0)),
            whole((ROWS, 16, 128)),
            whole((ROWS, 16, 128)),
        ],
        out_shape=[
            jax.ShapeDtypeStruct((73, 28, 16, 256), bf16),
            jax.ShapeDtypeStruct((ROWS, 16, 128), bf16),
            jax.ShapeDtypeStruct((ROWS, 16, 128), bf16),
        ],
        scratch_shapes=[pltpu.VMEM((ROWS + 8, 4, 16, 128), bf16)],
        cost_estimate=pl.CostEstimate(flops=2 * 2400 * 4 * 512 * 1024, bytes_accessed=24_000_000, transcendentals=0),
        name='main_first',
    )(top, mid, bot, toep, bias)


def edge_kernel(own0_ref, own5_ref, from_prev_ref, from_next_ref, toep_ref, bias_ref, left_ref, right_ref, slab_ref):
    step = pl.program_id(0)

    @pl.when(step == 0)
    def _():
        lane = lax.broadcasted_iota(jnp.int32, (16, 128), 1) % 32

        def merge(quad):
            for row in range(4):
                index = 4 * quad + row
                left = from_prev_ref[2 * quad + row // 2]
                if row % 2:
                    left = pltpu.roll(left, 128 - 16, 1)
                slab_ref[index, 0] = jnp.where(lane < 13, left, own0_ref[index])
                right = pltpu.roll(from_next_ref[quad], (1 - 8 * row) % 128, 1)
                slab_ref[index, 1] = jnp.where(lane < 1, own5_ref[index], right)

        blocked_loop(ROWS // 4, 8, merge)
        slab_ref[ROWS:ROWS + 8] = jnp.zeros((8, 2, 16, 128), jnp.bfloat16)

    bias = bias_ref[...]
    base = 4 * (PAIRS // STEPS) * step + 3

    def store(row, win, pair, value):
        ref = right_ref if win else left_ref
        ref[row // 2, pair, :, 128 * (row % 2):128 * (row % 2) + 128] = value

    for window in ((0, 7), (1, 2)):
        product(slab_ref, base, 2 * (PAIRS // STEPS), [window], toep_ref, bias, store)


def edge_first(own0, own5, from_prev, from_next, toep, bias):
    bf16 = jnp.bfloat16
    args = (own0, own5, from_prev, from_next, toep, bias)
    return pl.pallas_call(
        edge_kernel,
        grid=(STEPS,),
        in_specs=[whole(x.shape) for x in args],
        out_specs=[
            pl.BlockSpec((PAIRS // STEPS, 7, 16, 256), lambda s: (s, 0, 0, 0)),
            pl.BlockSpec((PAIRS // STEPS, 2, 16, 256), lambda s: (s, 0, 0, 0)),
        ],
        out_shape=[
            jax.ShapeDtypeStruct((73, 7, 16, 256), bf16),
            jax.ShapeDtypeStruct((73, 2, 16, 256), bf16),
        ],
        scratch_shapes=[pltpu.VMEM((ROWS + 8, 2, 16, 128), bf16)],
        cost_estimate=pl.CostEstimate(flops=2 * 2400 * 512 * 1152, bytes_accessed=12_000_000, transcendentals=0),
        name='edge_first',
    )(*args)


def rows_kernel(taps, rows, group, parts, *refs):
    x_refs, (w_ref, bias_ref, out_ref) = refs[:parts], refs[parts:]
    cols = out_ref.shape[1]

    @pl.loop(0, rows // group)
    def _(part):
        first = group * part
        lhs = []
        for row in range(group):
            slabs = [slab.reshape(cols * 16, slab.shape[-1]) for slab in taps(x_refs, first + row)]
            lhs.append(jnp.concatenate(slabs, axis=-1))
        lhs = jnp.concatenate(lhs, axis=0)
        acc = jnp.dot(lhs, w_ref[...], preferred_element_type=jnp.float32)
        acc = jnp.maximum(acc + bias_ref[...], 0.0).astype(jnp.bfloat16)
        out_ref[pl.ds(first, group)] = acc.reshape(group, cols, 16, 256)


def rows_conv(xs, weight, bias, taps, halo, grid, rows, group, cols, out_rows, first_cols):
    def window(x, cut):
        start, size = cut
        block = (pl.Element(rows + halo), pl.Element(size)) + tuple(pl.Element(n) for n in x.shape[2:])
        rest = (0,) * (len(x.shape) - 2)
        return pl.BlockSpec(block, lambda s: (rows * s, start) + rest)

    out_shape = jax.ShapeDtypeStruct((out_rows, cols, 16, 256), jnp.bfloat16)
    flops = 2 * grid * rows * cols * 16 * weight.shape[0] * 256
    return pl.pallas_call(
        functools.partial(rows_kernel, taps, rows, group, len(xs)),
        grid=(grid,),
        in_specs=[window(x, cut) for x, cut in zip(xs, first_cols)] + [whole(weight.shape), whole((1, 256))],
        out_specs=pl.BlockSpec((rows, cols, 16, 256), lambda s: (s, 0, 0, 0)),
        out_shape=out_shape,
        cost_estimate=pl.CostEstimate(flops=flops, bytes_accessed=40_000_000, transcendentals=0),
    )(*xs, weight, bias.reshape(1, 256))


def refine1_taps(refs, row):
    left, main, right = refs
    slabs = []
    for tap in range(2):
        at = row + tap
        slabs.append(jnp.concatenate([left[at], main[at], right[at, 0:1]], axis=0))
        slabs.append(jnp.concatenate([left[at, 1:7], main[at], right[at]], axis=0))
    return slabs


def down2_taps(refs, row):
    (pairs,) = refs
    slabs = []
    for tap in range(2):
        lanes = 256 if tap == 0 else 128
        even, odd = pairs[row + tap, :, 0, :, :lanes], pairs[row + tap, :, 1, :, :lanes]
        slabs += [jnp.concatenate([odd[:1], odd[:-1]], axis=0), even, odd]
    return slabs


def refine2_taps(refs, row):
    (x,) = refs
    cols = x.shape[1] - 1
    return [x[row + tap, part:part + cols] for tap in range(3) for part in range(2)]


def pack_first(weight):
    cols = []
    for out_col in range(OUT_COLS):
        cols.append(jnp.pad(weight, ((0, 0), (2 * out_col, 29 - 2 * out_col), (0, 0), (0, 0))))
    stacked = jnp.concatenate(cols, axis=-1)
    return stacked.transpose(0, 2, 1, 3).reshape(384, 64 * OUT_COLS)


def pack_refine1(weight):
    wide = jnp.pad(weight, ((1, 1), (1, 1), (0, 0), (0, 0)))
    pieces = [wide[1 - r:5 - r, 1 - c:5 - c] for r in range(2) for c in range(2)]
    joined = jnp.concatenate(pieces, axis=-1)
    return joined.reshape(2, 2, 2, 2, 64, 256).transpose(0, 2, 1, 3, 4, 5).reshape(2, 2, 256, 256)


def pack_down2(weight):
    wide = jnp.pad(weight, ((0, 1), (2, 3), (0, 0), (0, 0)))
    joined = jnp.concatenate([wide[:, 2:8], wide[:, 0:6]], axis=-1)
    return joined.reshape(2, 2, 3, 2, 64, 256).transpose(0, 2, 1, 3, 4, 5).reshape(2, 3, 256, 256)


def pack_refine2(weight):
    wide = jnp.pad(weight, ((0, 0), (1, 1), (0, 0), (0, 0)))
    joined = jnp.concatenate([wide[:, 1:5], wide[:, 0:4]], axis=-1)
    return joined.reshape(3, 2, 256, 256)


def pack_down3(weight):
    return jnp.pad(weight, ((0, 0), (1, 0), (0, 0), (0, 0))).reshape(3, 2, 256, 256)


def conv(x, weight, bias, strides=(1, 1), pads=((0, 0), (0, 0))):
    out = lax.conv_general_dilated(x, weight, strides, pads, dimension_numbers=DIM_NUMS, preferred_element_type=jnp.float32)
    return lax.optimization_barrier(jnp.maximum(out + bias, 0.0).astype(jnp.bfloat16))


def solution(mesh):
    h_count = mesh.shape['h']
    w_count = mesh.shape['w']
    tile_spec = P('batch', 'h', 'w', None)

    def per_device(images, dw1, db1, rw1, rb1, dw2, db2, rw2, rb2, dw3, db3, rw3, rb3):
        native = images.transpose(0, 1, 3, 2)
        top = lax.ppermute(native[:, -TOP:], 'h', next_perm(h_count))
        bot = lax.ppermute(native[:, :BOT], 'h', prev_perm(h_count))
        top, mid, bot = (x.transpose(1, 2, 0, 3) for x in (top, native, bot))
        toep = pack_first(dw1)
        bias1 = jnp.tile(db1, 4).reshape(1, 256)
        to_next, to_prev = pack_halo(top, mid, bot)
        to_next, rw1, rb1, dw2, db2, rw2, rb2, dw3 = lax.optimization_barrier((to_next, rw1, rb1, dw2, db2, rw2, rb2, dw3))
        from_prev = lax.ppermute(to_next, 'w', next_perm(w_count))
        from_next = lax.ppermute(to_prev, 'w', prev_perm(w_count))
        y1_main, own0, own5 = main_first(top, mid, bot, toep, bias1)
        y1_left, y1_right = edge_first(own0, own5, from_prev, from_next, toep, bias1)
        rw1, dw2 = pack_refine1(rw1).reshape(1024, 256), pack_down2(dw2)
        dw2 = jnp.concatenate([dw2[0].reshape(768, 256), dw2[1, :, :128].reshape(384, 256)], axis=0)
        z1 = rows_conv((y1_left, y1_main, y1_right), rw1, jnp.tile(rb1, 4), refine1_taps, 1, 9, 8, 4, 36, 73, ((0, 7), (0, 28), (0, 2)))
        z1 = z1.reshape(73, 18, 2, 16, 256)
        y2 = rows_conv((z1,), dw2, jnp.tile(db2, 2), down2_taps, 1, 9, 8, 8, 18, 72, ((0, 18),))
        rw2, rb2, dw3 = pack_refine2(rw2), jnp.tile(rb2, 2), pack_down3(dw3)
        y2_edge = jnp.concatenate([y2[:, :3], y2[:, 15:18]], axis=2)
        z2_edge = conv(y2_edge, rw2, rb2)
        y3_edge = conv(z2_edge, dw3, db3, (2, 1))
        y3_left, y3_right = y3_edge[:, :, :16], y3_edge[:, :, 16:]
        from_left = lax.ppermute(y3_right, 'w', next_perm(w_count))
        from_right = lax.ppermute(y3_left, 'w', prev_perm(w_count))
        y2, y3_edge = lax.optimization_barrier((y2, y3_edge))
        z2_mid = rows_conv((y2,), rw2.reshape(1536, 256), rb2, refine2_taps, 2, 7, 10, 10, 13, 70, ((2, 14),))
        z2 = jnp.concatenate([z2_edge[:, 1:2, :16], z2_mid, z2_edge[:, 0:1, 16:]], axis=1)
        y3_mid = conv(z2, dw3, db3, (2, 1))
        y3_left, y3_right = y3_edge[:, :, :16], y3_edge[:, :, 16:]
        y3_left = jnp.concatenate([from_left, y3_left], axis=1)
        y3_right = jnp.concatenate([y3_right, from_right], axis=1)
        y3_left, y3_right = lax.optimization_barrier((y3_left, y3_right))
        y3 = jnp.concatenate([y3_left, y3_mid, y3_right], axis=1)
        z3 = conv(y3, rw3, rb3)
        return z3.transpose(2, 0, 1, 3)

    in_specs = (tile_spec,) + (P(),) * 12
    return jax.shard_map(per_device, mesh=mesh, in_specs=in_specs, out_specs=tile_spec, check_vma=False)
```

```python
import functools

import jax
import jax.numpy as jnp
from jax import lax
from jax.experimental import pallas as pl
from jax.experimental.pallas import tpu as pltpu
from jax.sharding import PartitionSpec as P


DIM_NUMS = ('HWNC', 'HWIO', 'HWNC')

TOP, MID, BOT = 24, 256, 16
ROWS = TOP + MID + BOT
PAIRS = 75
STEPS = 3
STEP = 28
FIRST = -13
OUT_COLS = 14


def next_perm(axis_size):
    return [(src_dev, (src_dev + 1) % axis_size) for src_dev in range(axis_size)]


def prev_perm(axis_size):
    return [(src_dev, (src_dev - 1) % axis_size) for src_dev in range(axis_size)]


def lane_window(pieces, start, offset):
    lane = lax.broadcasted_iota(jnp.int32, pieces[0].shape, 1)
    total = None
    for chan, piece in enumerate(pieces):
        shift = (32 * chan + offset - start) % 128
        moved = pltpu.roll(piece, shift, 1) if shift else piece
        total = moved if total is None else jnp.where(lane >= 32 * chan, moved, total)
    return total


def blocked_loop(count, unroll, body):
    @pl.loop(0, count // unroll)
    def _(block):
        for part in range(unroll):
            body(unroll * block + part)

    for index in range(count - count % unroll, count):
        body(index)


def for_quads(sources, unroll, body):
    first = 0
    for source in sources:
        def one(quad, source=source, first=first):
            rows = [[source[4 * quad + row, chan] for chan in range(4)] for row in range(4)]
            body(first + quad, rows)

        blocked_loop(source.shape[0] // 4, unroll, one)
        first += source.shape[0] // 4


def pack_kernel(top_ref, mid_ref, bot_ref, to_next_ref, to_prev_ref):
    lane = lax.broadcasted_iota(jnp.int32, (16, 128), 1) % 32

    def body(quad, rows):
        last = [lane_window(rows[row], 115, 16 * (row % 2)) for row in range(4)]
        to_next_ref[2 * quad] = jnp.where(lane < 16, last[0], last[1])
        to_next_ref[2 * quad + 1] = jnp.where(lane < 16, last[2], last[3])
        packed = lane_window(rows[0], 0, 0)
        for row in range(1, 4):
            packed = jnp.where(lane >= 8 * row, lane_window(rows[row], 0, 8 * row), packed)
        to_prev_ref[quad] = packed

    for_quads((top_ref, mid_ref, bot_ref), 8, body)


def pack_halo(top, mid, bot):
    return pl.pallas_call(
        pack_kernel,
        out_shape=[
            jax.ShapeDtypeStruct((ROWS // 2, 16, 128), jnp.bfloat16),
            jax.ShapeDtypeStruct((ROWS // 4, 16, 128), jnp.bfloat16),
        ],
        cost_estimate=pl.CostEstimate(flops=8_000_000, bytes_accessed=6_000_000, transcendentals=0),
        name='pack',
    )(top, mid, bot)


def product(slab_ref, base, rows, windows, toep_ref, bias, store):
    lhs = []
    for row in range(rows):
        for win, _ in windows:
            taps = [slab_ref[base + 2 * row + tap, win] for tap in range(3)]
            lhs.append(jnp.concatenate(taps, axis=-1))
    lhs = jnp.concatenate(lhs, axis=0)
    most = max(count for _, count in windows)
    for chunk in range((most + 1) // 2):
        width = min(256, 128 * (most - 2 * chunk))
        acc = jnp.dot(lhs, toep_ref[:, 256 * chunk:256 * chunk + width], preferred_element_type=jnp.float32)
        acc = jnp.maximum(acc + bias[:, :width], 0.0).astype(jnp.bfloat16)
        acc = acc.reshape(rows, len(windows), 16, width)
        for index, (win, count) in enumerate(windows):
            for half in range(width // 128):
                pair = 2 * chunk + half
                if pair < count:
                    for row in range(rows):
                        store(row, win, pair, acc[row, index, :, 128 * half:128 * half + 128])


def main_kernel(top_ref, mid_ref, bot_ref, toep_ref, bias_ref, out_ref, own0_ref, own5_ref, slab_ref):
    step = pl.program_id(0)

    @pl.when(step == 0)
    def _():
        def body(quad, rows):
            for row in range(4):
                index = 4 * quad + row
                for win in range(4):
                    slab_ref[index, win] = lane_window(rows[row], FIRST + STEP * (win + 1), 0)
                own0_ref[index] = lane_window(rows[row], 0, 13)
                own5_ref[index] = lane_window(rows[row], 127, 0)

        for_quads((top_ref, mid_ref, bot_ref), 4, body)
        slab_ref[ROWS:ROWS + 8] = jnp.zeros((8, 4, 16, 128), jnp.bfloat16)

    bias = bias_ref[...]
    group = 5

    @pl.loop(0, PAIRS // STEPS // group)
    def _(part):
        first = group * part

        def store(row, win, pair, value):
            out_ref[first + row // 2, 7 * win + pair, :, 128 * (row % 2):128 * (row % 2) + 128] = value

        base = 4 * (PAIRS // STEPS * step + first) + 3
        product(slab_ref, base, 2 * group, [(win, 7) for win in range(4)], toep_ref, bias, store)


def whole(shape):
    return pl.BlockSpec(shape, lambda s: (0,) * len(shape), pipeline_mode=pl.Buffered(1))


def main_first(top, mid, bot, toep, bias):
    bf16 = jnp.bfloat16
    return pl.pallas_call(
        main_kernel,
        grid=(STEPS,),
        in_specs=[whole(x.shape) for x in (top, mid, bot, toep, bias)],
        out_specs=[
            pl.BlockSpec((PAIRS // STEPS, 28, 16, 256), lambda s: (s, 0, 0, 0)),
            whole((ROWS, 16, 128)),
            whole((ROWS, 16, 128)),
        ],
        out_shape=[
            jax.ShapeDtypeStruct((73, 28, 16, 256), bf16),
            jax.ShapeDtypeStruct((ROWS, 16, 128), bf16),
            jax.ShapeDtypeStruct((ROWS, 16, 128), bf16),
        ],
        scratch_shapes=[pltpu.VMEM((ROWS + 8, 4, 16, 128), bf16)],
        cost_estimate=pl.CostEstimate(flops=2 * 2400 * 4 * 512 * 1024, bytes_accessed=24_000_000, transcendentals=0),
        name='main_first',
    )(top, mid, bot, toep, bias)


def edge_kernel(own0_ref, own5_ref, from_prev_ref, from_next_ref, toep_ref, bias_ref, left_ref, right_ref, slab_ref):
    step = pl.program_id(0)

    @pl.when(step == 0)
    def _():
        lane = lax.broadcasted_iota(jnp.int32, (16, 128), 1) % 32

        def merge(quad):
            for row in range(4):
                index = 4 * quad + row
                left = from_prev_ref[2 * quad + row // 2]
                if row % 2:
                    left = pltpu.roll(left, 128 - 16, 1)
                slab_ref[index, 0] = jnp.where(lane < 13, left, own0_ref[index])
                right = pltpu.roll(from_next_ref[quad], (1 - 8 * row) % 128, 1)
                slab_ref[index, 1] = jnp.where(lane < 1, own5_ref[index], right)

        blocked_loop(ROWS // 4, 8, merge)
        slab_ref[ROWS:ROWS + 8] = jnp.zeros((8, 2, 16, 128), jnp.bfloat16)

    bias = bias_ref[...]
    base = 4 * (PAIRS // STEPS) * step + 3

    def store(row, win, pair, value):
        ref = right_ref if win else left_ref
        ref[row // 2, pair, :, 128 * (row % 2):128 * (row % 2) + 128] = value

    for window in ((0, 7), (1, 2)):
        product(slab_ref, base, 2 * (PAIRS // STEPS), [window], toep_ref, bias, store)


def edge_first(own0, own5, from_prev, from_next, toep, bias):
    bf16 = jnp.bfloat16
    args = (own0, own5, from_prev, from_next, toep, bias)
    return pl.pallas_call(
        edge_kernel,
        grid=(STEPS,),
        in_specs=[whole(x.shape) for x in args],
        out_specs=[
            pl.BlockSpec((PAIRS // STEPS, 7, 16, 256), lambda s: (s, 0, 0, 0)),
            pl.BlockSpec((PAIRS // STEPS, 2, 16, 256), lambda s: (s, 0, 0, 0)),
        ],
        out_shape=[
            jax.ShapeDtypeStruct((73, 7, 16, 256), bf16),
            jax.ShapeDtypeStruct((73, 2, 16, 256), bf16),
        ],
        scratch_shapes=[pltpu.VMEM((ROWS + 8, 2, 16, 128), bf16)],
        cost_estimate=pl.CostEstimate(flops=2 * 2400 * 512 * 1152, bytes_accessed=12_000_000, transcendentals=0),
        name='edge_first',
    )(*args)


def rows_kernel(taps, rows, group, parts, *refs):
    x_refs, (w_ref, bias_ref, out_ref) = refs[:parts], refs[parts:]
    cols = out_ref.shape[1]

    @pl.loop(0, rows // group)
    def _(part):
        first = group * part
        lhs = []
        for row in range(group):
            slabs = [slab.reshape(cols * 16, slab.shape[-1]) for slab in taps(x_refs, first + row)]
            lhs.append(jnp.concatenate(slabs, axis=-1))
        lhs = jnp.concatenate(lhs, axis=0)
        acc = jnp.dot(lhs, w_ref[...], preferred_element_type=jnp.float32)
        acc = jnp.maximum(acc + bias_ref[...], 0.0).astype(jnp.bfloat16)
        out_ref[pl.ds(first, group)] = acc.reshape(group, cols, 16, 256)


def rows_conv(xs, weight, bias, taps, halo, grid, rows, group, cols, out_rows, first_cols):
    def window(x, cut):
        start, size = cut
        block = (pl.Element(rows + halo), pl.Element(size)) + tuple(pl.Element(n) for n in x.shape[2:])
        rest = (0,) * (len(x.shape) - 2)
        return pl.BlockSpec(block, lambda s: (rows * s, start) + rest)

    out_shape = jax.ShapeDtypeStruct((out_rows, cols, 16, 256), jnp.bfloat16)
    flops = 2 * grid * rows * cols * 16 * weight.shape[0] * 256
    return pl.pallas_call(
        functools.partial(rows_kernel, taps, rows, group, len(xs)),
        grid=(grid,),
        in_specs=[window(x, cut) for x, cut in zip(xs, first_cols)] + [whole(weight.shape), whole((1, 256))],
        out_specs=pl.BlockSpec((rows, cols, 16, 256), lambda s: (s, 0, 0, 0)),
        out_shape=out_shape,
        cost_estimate=pl.CostEstimate(flops=flops, bytes_accessed=40_000_000, transcendentals=0),
    )(*xs, weight, bias)


def refine1_taps(refs, row):
    left, main, right = refs
    slabs = []
    for tap in range(2):
        at = row + tap
        slabs.append(jnp.concatenate([left[at], main[at], right[at, 0:1]], axis=0))
        slabs.append(jnp.concatenate([left[at, 1:7], main[at], right[at]], axis=0))
    return slabs


def down2_taps(refs, row):
    (pairs,) = refs
    slabs = []
    for tap in range(2):
        lanes = 256 if tap == 0 else 128
        even, odd = pairs[row + tap, :, 0, :, :lanes], pairs[row + tap, :, 1, :, :lanes]
        slabs += [jnp.concatenate([odd[:1], odd[:-1]], axis=0), even, odd]
    return slabs


def pack_first(weight):
    cols = []
    for out_col in range(OUT_COLS):
        cols.append(jnp.pad(weight, ((0, 0), (2 * out_col, 29 - 2 * out_col), (0, 0), (0, 0))))
    stacked = jnp.concatenate(cols, axis=-1)
    return stacked.transpose(0, 2, 1, 3).reshape(384, 64 * OUT_COLS)


def weights_kernel(rw1_ref, rb1_ref, dw2_ref, db2_ref, rw2_ref, rb2_ref, dw3_ref, rw1_out, rb1_out, dw2_out, db2_out, rw2_out, rb2_out, dw3_out):
    def tap(ref, a, b):
        if 0 <= a <= 2 and 0 <= b <= 2:
            return ref[a, b]
        return jnp.zeros(ref.shape[2:], ref.dtype)

    for big_a in range(2):
        for big_b in range(2):
            for r in range(2):
                for c in range(2):
                    row = 64 * (8 * big_a + 4 * big_b + 2 * r + c)
                    pieces = [tap(rw1_ref, 2 * big_a + r - r_out, 2 * big_b + c - c_out) for r_out in range(2) for c_out in range(2)]
                    rw1_out[row:row + 64] = jnp.concatenate(pieces, axis=-1)
    row = 0
    for big_a in range(2):
        for big_b in range(3):
            for r in range(2 - big_a):
                for c in range(2):
                    pieces = [tap(dw2_ref, 2 * big_a + r, 2 * big_b + c - 2 * c_out) for c_out in range(2)]
                    dw2_out[row:row + 64] = jnp.concatenate(pieces, axis=-1)
                    row += 64
    for a in range(3):
        for b in range(4):
            row = 128 * (4 * a + b)
            pieces = [tap(rw2_ref, a, b - c_out) for c_out in range(2)]
            rw2_out[row:row + 128] = jnp.concatenate(pieces, axis=-1)
            dw3_out[row:row + 128] = tap(dw3_ref, a, b - 1)
    rb1_out[...] = jnp.concatenate([rb1_ref[...]] * 4, axis=-1)
    db2_out[...] = jnp.concatenate([db2_ref[...]] * 2, axis=-1)
    rb2_out[...] = jnp.concatenate([rb2_ref[...]] * 2, axis=-1)


def pack_weights(rw1, rb1, dw2, db2, rw2, rb2, dw3):
    rows = (1024, 1, 1152, 1, 1536, 1, 1536)
    return pl.pallas_call(
        weights_kernel,
        out_shape=[jax.ShapeDtypeStruct((n, 256), jnp.float32 if n == 1 else jnp.bfloat16) for n in rows],
        cost_estimate=pl.CostEstimate(flops=4_000_000, bytes_accessed=5_000_000, transcendentals=0),
        name='weights',
    )(rw1, rb1.reshape(1, 64), dw2, db2.reshape(1, 128), rw2, rb2.reshape(1, 128), dw3)


def conv(x, weight, bias, strides=(1, 1), pads=((0, 0), (0, 0))):
    out = lax.conv_general_dilated(x, weight, strides, pads, dimension_numbers=DIM_NUMS, preferred_element_type=jnp.float32)
    return lax.optimization_barrier(jnp.maximum(out + bias, 0.0).astype(jnp.bfloat16))


def solution(mesh):
    h_count = mesh.shape['h']
    w_count = mesh.shape['w']
    tile_spec = P('batch', 'h', 'w', None)

    def per_device(images, dw1, db1, rw1, rb1, dw2, db2, rw2, rb2, dw3, db3, rw3, rb3):
        native = images.transpose(0, 1, 3, 2)
        top = lax.ppermute(native[:, -TOP:], 'h', next_perm(h_count))
        bot = lax.ppermute(native[:, :BOT], 'h', prev_perm(h_count))
        top, mid, bot = (x.transpose(1, 2, 0, 3) for x in (top, native, bot))
        toep = pack_first(dw1)
        bias1 = jnp.tile(db1, 4).reshape(1, 256)
        to_next, to_prev = pack_halo(top, mid, bot)
        to_next, rw1, rb1, dw2, db2, rw2, rb2, dw3 = lax.optimization_barrier((to_next, rw1, rb1, dw2, db2, rw2, rb2, dw3))
        from_prev = lax.ppermute(to_next, 'w', next_perm(w_count))
        from_next = lax.ppermute(to_prev, 'w', prev_perm(w_count))
        y1_main, own0, own5 = main_first(top, mid, bot, toep, bias1)
        y1_left, y1_right = edge_first(own0, own5, from_prev, from_next, toep, bias1)
        rw1, rb1, dw2, db2, rw2, rb2, dw3 = pack_weights(rw1, rb1, dw2, db2, rw2, rb2, dw3)
        rw2, dw3 = rw2.reshape(3, 2, 256, 256), dw3.reshape(3, 2, 256, 256)
        z1 = rows_conv((y1_left, y1_main, y1_right), rw1, rb1, refine1_taps, 1, 9, 8, 4, 36, 73, ((0, 7), (0, 28), (0, 2)))
        z1 = z1.reshape(73, 18, 2, 16, 256)
        y2 = rows_conv((z1,), dw2, db2, down2_taps, 1, 9, 8, 8, 18, 72, ((0, 18),))
        y2_edge = jnp.concatenate([y2[:, :3], y2[:, 15:18]], axis=2)
        z2_edge = conv(y2_edge, rw2, rb2)
        y3_edge = conv(z2_edge, dw3, db3, (2, 1))
        y3_left, y3_right = y3_edge[:, :, :16], y3_edge[:, :, 16:]
        from_left = lax.ppermute(y3_right, 'w', next_perm(w_count))
        from_right = lax.ppermute(y3_left, 'w', prev_perm(w_count))
        y2, y3_edge = lax.optimization_barrier((y2, y3_edge))
        z2_mid = conv(y2[:, 2:16], rw2, rb2)
        z2 = jnp.concatenate([z2_edge[:, 1:2, :16], z2_mid, z2_edge[:, 0:1, 16:]], axis=1)
        y3_mid = conv(z2, dw3, db3, (2, 1))
        y3_left, y3_right = y3_edge[:, :, :16], y3_edge[:, :, 16:]
        y3_left = jnp.concatenate([from_left, y3_left], axis=1)
        y3_right = jnp.concatenate([y3_right, from_right], axis=1)
        y3_left, y3_right = lax.optimization_barrier((y3_left, y3_right))
        y3 = jnp.concatenate([y3_left, y3_mid, y3_right], axis=1)
        z3 = conv(y3, rw3, rb3)
        return z3.transpose(2, 0, 1, 3)

    in_specs = (tile_spec,) + (P(),) * 12
    return jax.shard_map(per_device, mesh=mesh, in_specs=in_specs, out_specs=tile_spec, check_vma=False)
```
